32 devices in a mesh: phi: 8 (over z, core), gz: 4 (over y, x).
Axes of the slice: x: 2, y: 2, z: 4, core: 2. Of those that a mesh axis runs over, the one named last changes fastest.
Arguments:
- charge: float32 [1024, 64, 256], P('phi', 'gz'), may hold values from -24 to 24
- outer_held: int32 [64], replicated, may hold values 0 or 1
- end_held: int32 [256], replicated, may hold values 0 or 1
Outputs:
- potential: float32 [1024, 64, 256], P('phi', 'gz')
- scales: float32 [2, 1024], P(None, 'phi')
The draws below stay inside these ranges and needn't reach their ends.
Inputs may be any that keep to these rules, and one draw needn't show every extreme that they name: `outer_held`: 1 holds the boundary at zero potential, 0 leaves it without flux. `end_held`: 1 holds both z ends of the radial cell at zero potential, 0 leaves them without flux.
All inputs are finite; a program needn't handle non-finite values.
Results may differ from the reference program's by a relative error of at most 0.0003.
Values sent between devices are 32-bit elements; how exact they have to be, the bound alone decides.
No kernel may reach another device: no remote copies, remote signals or barrier semaphores. Data moves between devices by JAX's collectives and lax.ppermute only.
A program may use at most 128 MiB of HBM per device.

```python
import math
import jax
import jax.numpy as jnp
from jax import lax

NPHI = 1024
NR = 256
VCYC = 2
NU = 2
KC = 3
RIN = 131
NZ = 64


def set_ends(array, own_key, least, largest):
    place = [jax.random.randint(jax.random.fold_in(own_key, axis), (), 0, length) for axis, length in enumerate(array.shape)]
    longest = array.shape.index(max(array.shape))
    neighbour = place[:longest] + [(place[longest] + 1) % array.shape[longest]] + place[longest + 1:]
    return array.at[tuple(place)].set(least).at[tuple(neighbour)].set(largest)


def steps_of(own_key, dims, pieces, low, largest):
    gain, own = 1.0, jax.random.fold_in(own_key, 6)
    for dim, shards_of in pieces:
        heights = jnp.exp(jax.random.uniform(jax.random.fold_in(own, dim), (shards_of,), jnp.float32, low / len(pieces), largest / len(pieces)))
        gain = gain * jnp.repeat(heights, dims[dim] // shards_of).reshape([-1 if axis == dim else 1 for axis in range(len(dims))])
    return gain


def bell_draw(own_key, shape, scale, reach, pieces=(), kind=jnp.bfloat16):
    values = jax.random.normal(own_key, shape, jnp.float32) * scale
    if len(pieces) > 0:
        values = steps_of(own_key, shape, pieces, -0.22, 0.18) * values
    return jnp.clip(values, min=-reach, max=reach).astype(kind)


def setup_inputs(seed: int = 0) -> dict:
    key_of = jax.random.split(jax.random.key(seed), 4)
    return {
        "charge": bell_draw(key_of[0], (NPHI, NZ, NR), 4.0, 24.0, ((0, 8), (1, 4)), jnp.float32),
        "outer_held": set_ends((jax.random.randint(key_of[1], (NZ,), 0, 2) < 1).astype(jnp.int32), jax.random.fold_in(key_of[1], 1), 0, 1),
        "end_held": set_ends((jax.random.randint(key_of[2], (NR,), 0, 2) < 1).astype(jnp.int32), jax.random.fold_in(key_of[2], 1), 0, 1),
    }


relaxation = 0.8
small_floor = 1e-06

def hartley_table(length):
    row_ids = lax.broadcasted_iota(jnp.int32, (length, length), 0)
    col_ids = lax.broadcasted_iota(jnp.int32, (length, length), 1)
    phases = (row_ids * col_ids % length).astype(jnp.float32) * (2.0 * math.pi / length)
    return (jnp.cos(phases) + jnp.sin(phases)) * (1.0 / math.sqrt(length))

def transform_rows(hartley, values):
    flat = values.reshape(values.shape[0], -1)
    result = jnp.dot(hartley, flat, precision=lax.Precision.HIGHEST, preferred_element_type=jnp.float32)
    return result.reshape(values.shape)

def radial_terms(radial_count, coarse):
    position = jnp.arange(radial_count, dtype=jnp.float32)
    if coarse:
        radius = RIN + 2.0 * position + 1.0
        return (radius, (radius - 1.0) / (4.0 * radius), (radius + 1.0) / (4.0 * radius), 0.25)
    radius = RIN + position + 0.5
    return (radius, (radius - 0.5) / radius, (radius + 0.5) / radius, 1.0)

def diagonal(mode_ids, axial_ids, total_axial, radial, outer_bc, end_bc):
    radius, inward, outward, axial = radial
    last_radial = radius.shape[0] - 1
    radial_ids = jnp.arange(radius.shape[0], dtype=jnp.int32)
    open_out = (radial_ids[None, :] == last_radial) & (outer_bc[:, None] == 0)
    open_low = (axial_ids[:, None] == 0) & (end_bc[None, :] == 0)
    open_high = (axial_ids[:, None] == total_axial - 1) & (end_bc[None, :] == 0)
    baseline = inward[None, :] + outward[None, :] * jnp.where(open_out, 0.0, 1.0)
    baseline = baseline + axial * (jnp.where(open_low, 0.0, 1.0) + jnp.where(open_high, 0.0, 1.0))
    mode_order = jnp.minimum(mode_ids, NPHI - mode_ids).astype(jnp.float32)
    return baseline[None] + (mode_order * mode_order)[:, None, None] / (radius * radius)[None, None, :]

def neighbours(extended, radial):
    radius, inward, outward, axial = radial
    middle = extended[:, 1:-1, :]
    zero_edge = jnp.zeros_like(middle[:, :, :1])
    below_r = jnp.concatenate([zero_edge, middle[:, :, :-1]], axis=2)
    above_r = jnp.concatenate([middle[:, :, 1:], zero_edge], axis=2)
    return axial * (extended[:, 2:, :] + extended[:, :-2, :]) + inward * below_r + outward * above_r

def relax_step(extended, source, diag_part, radial):
    middle = extended[:, 1:-1, :]
    return middle + relaxation * (source + neighbours(extended, radial) - diag_part * middle) / diag_part

def operate(extended, diag_part, radial):
    return diag_part * extended[:, 1:-1, :] - neighbours(extended, radial)

def pad_axial(values):
    return jnp.pad(values, ((0, 0), (1, 1), (0, 0)))

def restrict(residual):
    modes, cells_z, cells_r = residual.shape
    return residual.reshape(modes, cells_z // 2, 2, cells_r // 2, 2).sum(axis=(2, 4)) * 0.25

def prolong(correction):
    return jnp.repeat(jnp.repeat(correction, 2, axis=1), 2, axis=2)

def solve_block(spectrum, first_mode, outer_held, end_held):
    mode_ids = first_mode + jnp.arange(spectrum.shape[0], dtype=jnp.int32)
    fine_terms = radial_terms(NR, False)
    coarse_terms = radial_terms(NR // 2, True)
    fine_diag = diagonal(mode_ids, jnp.arange(NZ, dtype=jnp.int32), NZ, fine_terms, outer_held, end_held)
    coarse_diag = diagonal(mode_ids, jnp.arange(NZ // 2, dtype=jnp.int32), NZ // 2, coarse_terms, outer_held[0::2], end_held[0::2])
    solution = jnp.zeros_like(spectrum)
    scale_rows = []
    for cycle_index in range(VCYC):
        for sweep_index in range(NU):
            solution = relax_step(pad_axial(solution), spectrum, fine_diag, fine_terms)
        residual = spectrum - operate(pad_axial(solution), fine_diag, fine_terms)
        coarse_rhs = restrict(residual)
        estimate = relaxation * coarse_rhs / coarse_diag
        for sweep_index in range(KC):
            estimate = relax_step(pad_axial(estimate), coarse_rhs, coarse_diag, coarse_terms)
        spread = prolong(estimate)
        image = operate(pad_axial(spread), fine_diag, fine_terms)
        top = lax.optimization_barrier(jnp.sum(residual * image, axis=(1, 2)))
        bottom = lax.optimization_barrier(jnp.sum(image * image, axis=(1, 2)))
        factor = top / (bottom + small_floor)
        solution = solution + factor[:, None, None] * spread
        for sweep_index in range(NU):
            solution = relax_step(pad_axial(solution), spectrum, fine_diag, fine_terms)
        scale_rows.append(factor)
    return (solution, jnp.stack(scale_rows))

def reference(charge, outer_held, end_held):
    hartley = hartley_table(NPHI)
    spectrum = transform_rows(hartley, charge)
    mode_block = math.gcd(NPHI, 64)
    count_blocks = NPHI // mode_block
    starts = jnp.arange(count_blocks, dtype=jnp.int32) * mode_block
    blocks = spectrum.reshape(count_blocks, mode_block, NZ, NR)

    def solve_one(inputs_pair):
        return solve_block(inputs_pair[0], inputs_pair[1], outer_held, end_held)
    solution, scales = lax.map(solve_one, (blocks, starts))
    solution = solution.reshape(NPHI, NZ, NR)
    scales = jnp.transpose(scales, (1, 0, 2)).reshape(VCYC, NPHI)
    potential = transform_rows(hartley, solution)
    return (potential, scales)
```

```python
import functools
import math

import jax
import jax.numpy as jnp
import numpy as np
from jax import lax
from jax.experimental import pallas as pl
from jax.experimental.pallas import tpu as pltpu
from jax.sharding import PartitionSpec as P

VCYC = 2
NU = 2
KC = 3
RIN = 131

relaxation = 0.8
small_floor = 1e-06

VMEM_LIMIT = 60 * 1024 * 1024


def split_bf16(values):
    high = values.astype(jnp.bfloat16)
    low = (values - high.astype(jnp.float32)).astype(jnp.bfloat16)
    return high, low


def hartley_halves(length):
    half = length // 2
    modes = np.arange(half)[:, None]
    cells = np.arange(half)[None, :]
    tables = []
    for parity in range(2):
        phases = ((2 * modes + parity) * cells % length) * (2.0 * math.pi / length)
        tables.append((np.cos(phases) + np.sin(phases)) / math.sqrt(length))
    exact = np.stack(tables)
    high = exact.astype(jnp.bfloat16)
    low = (exact - high.astype(np.float64)).astype(jnp.bfloat16)
    return np.stack([high, low], axis=1)


def parity_order(cells):
    order = np.concatenate([np.arange(0, cells, 2), np.arange(1, cells, 2)])
    matrix = np.zeros((cells, cells), np.float32)
    matrix[order, np.arange(cells)] = 1.0
    return matrix.astype(jnp.bfloat16)


def dot32(left, right):
    return jnp.dot(left, right, preferred_element_type=jnp.float32)


def three_dots(table_high, table_low, high, low):
    return dot32(table_high, high) + (dot32(table_high, low) + dot32(table_low, high))


def permuted_split(values, order):
    high, low = split_bf16(values)
    return dot32(high, order).astype(jnp.bfloat16), dot32(low, order).astype(jnp.bfloat16)


def forward_kernel(cells_ref, table_ref, order_ref, out_ref):
    sources, _, rows, cells_r = cells_ref.shape
    whole = cells_ref[...].reshape(sources * rows, cells_r)
    half = whole.shape[0] // 2
    for parity in range(2):
        mixed = whole[:half] + whole[half:] if parity == 0 else whole[:half] - whole[half:]
        high, low = permuted_split(mixed, order_ref[...])
        out_ref[0, parity] = three_dots(table_ref[parity, 0], table_ref[parity, 1], high, low)


def forward_transform(cells, tables, order):
    sources, rows_z, rows, cells_r = cells.shape
    half = sources * rows // 2
    return pl.pallas_call(
        forward_kernel,
        grid=(rows_z,),
        in_specs=[
            pl.BlockSpec((sources, 1, rows, cells_r), lambda z: (0, z, 0, 0)),
            pl.BlockSpec(tables.shape, lambda z: (0, 0, 0, 0)),
            pl.BlockSpec(order.shape, lambda z: (0, 0)),
        ],
        out_specs=pl.BlockSpec((1, 2, half, cells_r), lambda z: (z, 0, 0, 0)),
        out_shape=jax.ShapeDtypeStruct((rows_z, 2, half, cells_r), jnp.float32),
        compiler_params=pltpu.CompilerParams(vmem_limit_bytes=VMEM_LIMIT),
        name="forward_transform",
    )(cells, tables, order)


def backward_kernel(modes_ref, table_ref, order_ref, out_ref):
    dests, _, rows, cells_r = out_ref.shape
    half = dests * rows // 2
    parts = []
    for parity in range(2):
        high, low = permuted_split(modes_ref[0, parity], order_ref[...])
        parts.append(three_dots(table_ref[parity, 0], table_ref[parity, 1], high, low))
    out_ref[: dests // 2, 0] = (parts[0] + parts[1]).reshape(dests // 2, rows, cells_r)
    out_ref[dests // 2 :, 0] = (parts[0] - parts[1]).reshape(dests // 2, rows, cells_r)


def backward_transform(modes, tables, order, dests):
    rows_z, _, half, cells_r = modes.shape
    rows = 2 * half // dests
    return pl.pallas_call(
        backward_kernel,
        grid=(rows_z,),
        in_specs=[
            pl.BlockSpec((1, 2, half, cells_r), lambda z: (z, 0, 0, 0)),
            pl.BlockSpec(tables.shape, lambda z: (0, 0, 0, 0)),
            pl.BlockSpec(order.shape, lambda z: (0, 0)),
        ],
        out_specs=pl.BlockSpec((dests, 1, rows, cells_r), lambda z: (0, z, 0, 0)),
        out_shape=jax.ShapeDtypeStruct((dests, rows_z, rows, cells_r), jnp.float32),
        compiler_params=pltpu.CompilerParams(vmem_limit_bytes=VMEM_LIMIT),
        name="backward_transform",
    )(modes, tables, order)


def block_of(count, most):
    block = most
    while count % block:
        block //= 2
    return block


def solve_kernel(outer_ref, source_ref, order2_ref, ends_ref, out_ref, scale_ref,
                 ping, pong, rest, fine_w, fine_d, fine_g, rhs, thin, thick, coarse_w):
    total_z, modes, cells_r = source_ref.shape
    lanes = cells_r // 2
    total_y = total_z // 2
    tile = min(8, modes)
    tiles = modes // tile
    block_z = block_of(total_z, 8)
    block_y = block_of(total_y, 4)

    spot = lax.broadcasted_iota(jnp.int32, (1, lanes), 1)
    position = spot.astype(jnp.float32)
    first = spot == 0
    last = spot == lanes - 1
    fine = []
    for parity in range(2):
        radius = RIN + (2.0 * position + parity) + 0.5
        fine.append((radius, (radius - 0.5) / radius, (radius + 0.5) / radius))
    coarse_radius = RIN + 2.0 * position + 1.0
    coarse_in = (coarse_radius - 1.0) / (4.0 * coarse_radius)
    coarse_out = (coarse_radius + 1.0) / (4.0 * coarse_radius)
    in_even = jnp.where(first, 0.0, fine[0][1])
    out_even = fine[0][2]
    in_odd = fine[1][1]
    out_odd = jnp.where(last, 0.0, fine[1][2])
    coarse_below = jnp.where(first, 0.0, coarse_in)
    coarse_above = jnp.where(last, 0.0, coarse_out)

    order2 = order2_ref[...]
    for held in range(2):
        for end in range(2):
            variant = held + 2 * end
            for parity in range(2):
                radius, inward, outward = fine[parity]
                open_ends = jnp.where(ends_ref[:, parity * lanes:(parity + 1) * lanes] == 0, 1.0, 0.0)
                base = inward + outward
                if held == 0 and parity == 1:
                    base = inward + jnp.where(last, 0.0, outward)
                base = base + 2.0
                if end:
                    base = base - (2.0 * open_ends if total_z == 1 else open_ends)
                full = base + order2 / (radius * radius)
                there = slice(parity * lanes, (parity + 1) * lanes)
                fine_d[variant, :, there] = full
                fine_w[variant, :, there] = relaxation / full
                fine_g[variant, :, there] = full - 1.0 - (fine[0][2] if parity == 0 else fine[1][1])
            open_ends = jnp.where(ends_ref[:, :lanes] == 0, 0.25, 0.0)
            base = coarse_in + (jnp.where(last, 0.0, coarse_out) if held == 0 else coarse_out)
            base = base + 0.5
            if end:
                base = base - (2.0 * open_ends if total_y == 1 else open_ends)
            coarse_w[variant] = relaxation / (base + order2 / (coarse_radius * coarse_radius))

    zero_fine = jnp.zeros((1, modes, cells_r), jnp.float32)
    zero_coarse = jnp.zeros((1, modes, lanes), jnp.float32)
    for buffer in (ping, pong):
        buffer[pl.ds(0, 1)] = zero_fine
        buffer[pl.ds(total_z + 1, 1)] = zero_fine
    for buffer in (rhs, thin, thick):
        buffer[pl.ds(0, 1)] = zero_coarse
        buffer[pl.ds(total_y + 1, 1)] = zero_coarse

    def fine_variant(z):
        ends = jnp.where((z == 0) | (z == total_z - 1), 2, 0)
        return outer_ref[z] + ends

    def coarse_variant(y):
        ends = jnp.where((y == 0) | (y == total_y - 1), 2, 0)
        return outer_ref[2 * y] + ends

    even = pl.ds(0, lanes)
    odd = pl.ds(lanes, lanes)

    def each_fine(body):
        for step in range(tiles):
            there = pl.ds(step * tile, tile)

            def one(block, carry, there=there):
                body(block * block_z, there)
                return carry

            lax.fori_loop(0, total_z // block_z, one, 0)

    def each_coarse(body):
        for step in range(tiles):
            there = pl.ds(step * tile, tile)

            def one(block, carry, there=there):
                body(block * block_y, there)
                return carry

            lax.fori_loop(0, total_y // block_y, one, 0)

    def neighbour_sum(rows, at):
        before_e, before_o = rows[at - 1]
        here_e, here_o = rows[at]
        after_e, after_o = rows[at + 1]
        sum_e = (before_e + after_e) + (in_even * pltpu.roll(here_o, 1, 1) + out_even * here_o)
        sum_o = (before_o + after_o) + (in_odd * here_e + out_odd * pltpu.roll(here_e, lanes - 1, 1))
        return sum_e, sum_o

    def relax_rows(rows, z0, there, store):
        for at in range(block_z):
            z = z0 + at
            variant = fine_variant(z)
            sum_e, sum_o = neighbour_sum(rows, at + 1)
            here_e, here_o = rows[at + 1]
            new_e = (1.0 - relaxation) * here_e + fine_w[variant, there, even] * (source_ref[z, there, even] + sum_e)
            new_o = (1.0 - relaxation) * here_o + fine_w[variant, there, odd] * (source_ref[z, there, odd] + sum_o)
            store(z, there, new_e, new_o)

    def store_padded(buffer):
        def store(z, there, new_e, new_o):
            buffer[z + 1, there, even] = new_e
            buffer[z + 1, there, odd] = new_o
        return store

    def store_out(z, there, new_e, new_o):
        out_ref[z, there, even] = new_e
        out_ref[z, there, odd] = new_o

    def padded_rows(buffer, z0, there):
        return [(buffer[z0 + at, there, even], buffer[z0 + at, there, odd]) for at in range(block_z + 2)]

    def sweep(buffer, store):
        def body(z0, there):
            relax_rows(padded_rows(buffer, z0, there), z0, there, store)
        each_fine(body)

    def first_sweeps(store):
        def body(z0, there):
            rows = []
            for at in range(-1, block_z + 1):
                z = jnp.clip(z0 + at, 0, total_z - 1)
                variant = fine_variant(z)
                row_e = fine_w[variant, there, even] * source_ref[z, there, even]
                row_o = fine_w[variant, there, odd] * source_ref[z, there, odd]
                if at in (-1, block_z):
                    inside = jnp.where((z0 + at >= 0) & (z0 + at < total_z), 1.0, 0.0)
                    row_e = row_e * inside
                    row_o = row_o * inside
                rows.append((row_e, row_o))
            relax_rows(rows, z0, there, store)
        each_fine(body)

    def residual_pass(buffer):
        def body(z0, there):
            rows = padded_rows(buffer, z0, there)
            pair = None
            for at in range(block_z):
                z = z0 + at
                variant = fine_variant(z)
                sum_e, sum_o = neighbour_sum(rows, at + 1)
                here_e, here_o = rows[at + 1]
                left_e = (source_ref[z, there, even] + sum_e) - fine_d[variant, there, even] * here_e
                left_o = (source_ref[z, there, odd] + sum_o) - fine_d[variant, there, odd] * here_o
                rest[z, there, even] = left_e
                rest[z, there, odd] = left_o
                if at % 2 == 0:
                    pair = left_e + left_o
                else:
                    rhs[z0 // 2 + at // 2 + 1, there] = 0.25 * (pair + (left_e + left_o))
        each_fine(body)

    def coarse_rows(load, y0, there):
        return [load(y0 + at, there) for at in range(block_y + 2)]

    def coarse_relax(load, target):
        def body(y0, there):
            rows = coarse_rows(load, y0, there)
            for at in range(block_y):
                y = y0 + at
                here = rows[at + 1]
                total = 0.25 * (rows[at] + rows[at + 2]) + (
                    coarse_below * pltpu.roll(here, 1, 1) + coarse_above * pltpu.roll(here, lanes - 1, 1))
                weight = coarse_w[coarse_variant(y), there]
                target[y + 1, there] = (1.0 - relaxation) * here + weight * (rhs[y + 1, there] + total)
        each_coarse(body)

    def load_of(buffer):
        return lambda y, there: buffer[y, there]

    def load_first(y, there):
        inner = jnp.clip(y - 1, 0, total_y - 1)
        return coarse_w[coarse_variant(inner), there] * rhs[y, there]

    def coarse_solve():
        buffers = (thin, thick)
        load = load_first
        for step in range(KC):
            target = buffers[step % 2]
            coarse_relax(load, target)
            load = load_of(target)
        return buffers[(KC - 1) % 2]

    def image_scale(estimate, there):
        def one(block, carry):
            top, bottom = carry
            y0 = block * block_y
            rows = coarse_rows(load_of(estimate), y0, there)
            for at in range(block_y):
                here = rows[at + 1]
                side_e = in_even * pltpu.roll(here, 1, 1)
                side_o = out_odd * pltpu.roll(here, lanes - 1, 1)
                for low in range(2):
                    z = 2 * (y0 + at) + low
                    variant = fine_variant(z)
                    across = rows[at + 2 * low]
                    image_e = fine_g[variant, there, even] * here - (side_e + across)
                    image_o = fine_g[variant, there, odd] * here - (side_o + across)
                    top = top + (rest[z, there, even] * image_e + rest[z, there, odd] * image_o)
                    bottom = bottom + (image_e * image_e + image_o * image_o)
            return top, bottom

        nothing = jnp.zeros((tile, lanes), jnp.float32)
        top, bottom = lax.fori_loop(0, total_y // block_y, one, (nothing, nothing))
        top = jnp.sum(top, axis=1, keepdims=True)
        bottom = jnp.sum(bottom, axis=1, keepdims=True)
        return jnp.broadcast_to(top / (bottom + small_floor), (tile, lanes))

    def corrected_sweep(buffer, estimate, cycle, store):
        for step in range(tiles):
            there = pl.ds(step * tile, tile)
            scale = image_scale(estimate, there)
            scale_ref[cycle, there] = scale

            def one(block, carry, there=there, scale=scale):
                z0 = block * block_z
                rows = padded_rows(buffer, z0, there)
                added = []
                for at in range(-1, block_z // 2 + 1):
                    added.append(scale * estimate[z0 // 2 + at + 1, there])
                moved = []
                for at in range(block_z + 2):
                    plus = added[(at + 1) // 2]
                    moved.append((rows[at][0] + plus, rows[at][1] + plus))
                relax_rows(moved, z0, there, store)
                return carry

            lax.fori_loop(0, total_z // block_z, one, 0)

    for cycle in range(VCYC):
        if cycle == 0:
            first_sweeps(store_padded(ping))
            left = NU - 2
        else:
            left = NU
        here, other = ping, pong
        for _ in range(left):
            sweep(here, store_padded(other))
            here, other = other, here
        residual_pass(here)
        estimate = coarse_solve()
        for step in range(NU):
            final = cycle == VCYC - 1 and step == NU - 1
            store = store_out if final else store_padded(other)
            if step == 0:
                corrected_sweep(here, estimate, cycle, store)
            else:
                sweep(here, store)
            here, other = other, here
        ping, pong = here, other


def solve_modes(source, order2, outer_held, ends):
    total_z, modes, cells_r = source.shape
    lanes = cells_r // 2
    f32 = jnp.float32
    whole = pl.BlockSpec(memory_space=pltpu.VMEM)
    return pl.pallas_call(
        solve_kernel,
        in_specs=[pl.BlockSpec(memory_space=pltpu.SMEM), whole, whole, whole],
        out_specs=[whole, whole],
        out_shape=[
            jax.ShapeDtypeStruct((total_z, modes, cells_r), f32),
            jax.ShapeDtypeStruct((VCYC, modes, lanes), f32),
        ],
        scratch_shapes=[
            pltpu.VMEM((total_z + 2, modes, cells_r), f32),
            pltpu.VMEM((total_z + 2, modes, cells_r), f32),
            pltpu.VMEM((total_z, modes, cells_r), f32),
            pltpu.VMEM((4, modes, cells_r), f32),
            pltpu.VMEM((4, modes, cells_r), f32),
            pltpu.VMEM((4, modes, cells_r), f32),
            pltpu.VMEM((total_z // 2 + 2, modes, lanes), f32),
            pltpu.VMEM((total_z // 2 + 2, modes, lanes), f32),
            pltpu.VMEM((total_z // 2 + 2, modes, lanes), f32),
            pltpu.VMEM((4, modes, lanes), f32),
        ],
        compiler_params=pltpu.CompilerParams(vmem_limit_bytes=VMEM_LIMIT),
        name="solve_modes",
    )(outer_held, source, order2, ends)


def body(charge, outer_held, end_held):
    phi_size = lax.axis_size("phi")
    gz_size = lax.axis_size("gz")
    devices = phi_size * gz_size
    rows, cells_z, cells_r = charge.shape
    length = rows * phi_size
    rows_z = cells_z // phi_size
    total_z = cells_z * gz_size
    few = length // devices

    exact = hartley_halves(length)
    forward = jnp.asarray(exact)
    backward = lax.optimization_barrier(forward)
    backward = jnp.stack([backward[0], jnp.swapaxes(backward[1], 1, 2)])
    order = jnp.asarray(parity_order(cells_r))
    disorder = jnp.asarray(parity_order(cells_r).T)

    blocks = jnp.transpose(charge, (1, 0, 2)).reshape(phi_size, rows_z, rows, cells_r)
    blocks = lax.all_to_all(blocks, "phi", split_axis=0, concat_axis=0, tiled=True)
    modes = forward_transform(blocks, forward, order)

    modes = modes.reshape(rows_z, 2, phi_size, gz_size, few // 2, cells_r)
    modes = jnp.transpose(modes, (3, 2, 0, 1, 4, 5)).reshape(devices, rows_z, few, cells_r)
    own = lax.all_to_all(modes, ("gz", "phi"), split_axis=0, concat_axis=0, tiled=True)
    own = own.reshape(total_z, few, cells_r)

    place = lax.axis_index("phi") * gz_size + lax.axis_index("gz")
    slots = jnp.arange(few, dtype=jnp.int32)
    own_modes = place * few + 2 * (slots % (few // 2)) + slots // (few // 2)
    mode_order = jnp.minimum(own_modes, length - own_modes).astype(jnp.float32)
    order2 = (mode_order * mode_order)[:, None]
    ends = jnp.concatenate([end_held[0::2], end_held[1::2]])[None, :]
    solved, scale_lanes = solve_modes(own, order2, outer_held, ends)

    natural = scale_lanes[:, :, 0].reshape(VCYC, 2, few // 2)
    natural = jnp.transpose(natural, (0, 2, 1)).reshape(VCYC, few)
    scales = lax.all_gather(natural, "gz", axis=1, tiled=True)

    back = solved.reshape(devices, rows_z, few, cells_r)
    back = lax.all_to_all(back, ("gz", "phi"), split_axis=0, concat_axis=0, tiled=True)
    back = back.reshape(gz_size, phi_size, rows_z, 2, few // 2, cells_r)
    back = jnp.transpose(back, (2, 3, 1, 0, 4, 5)).reshape(rows_z, 2, length // 2, cells_r)
    cells = backward_transform(back, backward, disorder, phi_size)
    cells = lax.all_to_all(cells, "phi", split_axis=0, concat_axis=0, tiled=True)
    potential = jnp.transpose(cells.reshape(cells_z, rows, cells_r), (1, 0, 2))
    return (potential, scales)


def solution(mesh):
    in_specs = (P("phi", "gz", None), P(), P())
    out_specs = (P("phi", "gz", None), P(None, "phi"))
    return jax.shard_map(body, mesh=mesh, in_specs=in_specs, out_specs=out_specs, check_vma=False)
```

```python
import functools
import math

import jax
import jax.numpy as jnp
import numpy as np
from jax import lax
from jax.experimental import pallas as pl
from jax.experimental.pallas import tpu as pltpu
from jax.sharding import PartitionSpec as P

VCYC = 2
NU = 2
KC = 3
RIN = 131

relaxation = 0.8
small_floor = 1e-06

VMEM_LIMIT = 67043328


def split_bf16(values):
    high = values.astype(jnp.bfloat16)
    low = (values - high.astype(jnp.float32)).astype(jnp.bfloat16)
    return high, low


def block_of(count, most):
    block = most
    while count % block:
        block //= 2
    return block

def hartley_halves(length):
    half = length // 2
    modes = np.arange(half)[:, None]
    cells = np.arange(half)[None, :]
    tables = []
    for parity in range(2):
        phases = ((2 * modes + parity) * cells % length) * (2.0 * math.pi / length)
        tables.append((np.cos(phases) + np.sin(phases)) / math.sqrt(length))
    exact = np.stack(tables)
    high = exact.astype(jnp.bfloat16)
    low = (exact - high.astype(np.float64)).astype(jnp.bfloat16)
    return np.stack([high, low], axis=1)


def parity_order(cells):
    order = np.concatenate([np.arange(0, cells, 2), np.arange(1, cells, 2)])
    matrix = np.zeros((cells, cells), np.float32)
    matrix[order, np.arange(cells)] = 1.0
    return matrix.astype(jnp.bfloat16)


def dot32(left, right):
    return jnp.dot(left, right, preferred_element_type=jnp.float32)


def three_dots(table_high, table_low, high, low):
    return dot32(table_high, high) + (dot32(table_high, low) + dot32(table_low, high))


def permuted_split(values, order):
    high, low = split_bf16(values)
    return dot32(high, order).astype(jnp.bfloat16), dot32(low, order).astype(jnp.bfloat16)


def any_spec(array):
    rank = array.ndim
    return pl.BlockSpec(array.shape, lambda *_: (0,) * rank)


def f32_shape(*shape):
    return jax.ShapeDtypeStruct(shape, jnp.float32)


def sliced_cost(flops, *shapes):
    moved = 4 * sum(math.prod(shape) for shape in shapes)
    return pl.CostEstimate(flops=flops, bytes_accessed=moved, transcendentals=0)


def placed_after(kernel):
    return lambda me_ref, _, *refs: kernel(me_ref, *refs)


def params():
    return pltpu.CompilerParams(vmem_limit_bytes=VMEM_LIMIT)


def arrange_kernel(chunks, size, me_ref, cells_ref, *refs):
    out_refs, turned = refs[:-1], refs[-1]
    turned[...] = jnp.swapaxes(cells_ref[...], 0, 1)
    rows_z = turned.shape[0] // size
    at = 0
    for start, count, spread in chunks:
        if spread:
            for step in range(size):
                dest = lax.rem(me_ref[0] + step, size)
                for row in range(count):
                    out_refs[at + step][row] = turned[dest * rows_z + start + row]
            at += size
        else:
            for dest in range(size):
                for row in range(count):
                    out_refs[at][dest, row] = turned[dest * rows_z + start + row]
            at += 1


def arrange_cells(me, charge, chunks, size):
    rows, cells_z, cells_r = charge.shape
    part = block_of(rows, 32)
    shapes, specs = [], []
    for _, count, spread in chunks:
        if spread:
            shapes += [f32_shape(count, rows, cells_r)] * size
            specs += [pl.BlockSpec((count, part, cells_r), lambda p: (0, p, 0))] * size
        else:
            shapes.append(f32_shape(size, count, rows, cells_r))
            specs.append(pl.BlockSpec((size, count, part, cells_r), lambda p: (0, 0, p, 0)))
    outs = pl.pallas_call(
        functools.partial(arrange_kernel, chunks, size),
        grid=(rows // part,),
        in_specs=[
            pl.BlockSpec(memory_space=pltpu.SMEM),
            pl.BlockSpec((part, cells_z, cells_r), lambda p: (p, 0, 0)),
        ],
        out_specs=specs,
        out_shape=shapes,
        scratch_shapes=[pltpu.VMEM((cells_z, part, cells_r), jnp.float32)],
        compiler_params=params(),
        cost_estimate=sliced_cost(charge.size, charge.shape, charge.shape),
        name="arrange_cells",
    )(me, charge)
    return split_chunks(outs, chunks, size)


def split_chunks(arrays, chunks, size):
    result, at = [], 0
    for _, _, spread in chunks:
        width = size if spread else 1
        result.append(list(arrays[at:at + width]))
        at += width
    return result


def gather_kernel(chunks, size, me_ref, *refs):
    in_refs, out_ref, turned = refs[:-2], refs[-2], refs[-1]
    rows_z = turned.shape[0] // size
    for (start, count, spread), group in zip(chunks, split_chunks(in_refs, chunks, size)):
        for step in range(size):
            if spread:
                source = lax.rem(me_ref[0] + size - step, size)
                for row in range(count):
                    turned[source * rows_z + start + row] = group[step][row]
            else:
                for row in range(count):
                    turned[step * rows_z + start + row] = group[0][step, row]
    out_ref[...] = jnp.swapaxes(turned[...], 0, 1)


def gather_cells(me, groups, chunks, size, rows, cells_z, cells_r):
    part = block_of(rows, 32)
    specs = []
    for _, count, spread in chunks:
        if spread:
            specs += [pl.BlockSpec((count, part, cells_r), lambda p: (0, p, 0))] * size
        else:
            specs.append(pl.BlockSpec((size, count, part, cells_r), lambda p: (0, 0, p, 0)))
    shape = (rows, cells_z, cells_r)
    return pl.pallas_call(
        functools.partial(gather_kernel, chunks, size),
        grid=(rows // part,),
        in_specs=[pl.BlockSpec(memory_space=pltpu.SMEM)] + specs,
        out_specs=pl.BlockSpec((part, cells_z, cells_r), lambda p: (p, 0, 0)),
        out_shape=f32_shape(*shape),
        scratch_shapes=[pltpu.VMEM((cells_z, part, cells_r), jnp.float32)],
        compiler_params=params(),
        cost_estimate=sliced_cost(math.prod(shape), shape, shape),
        name="gather_cells",
    )(me, *[array for group in groups for array in group])


def forward_kernel(size, me_ref, *refs):
    in_refs, table_ref, order_ref, out_ref, whole = refs[:-4], refs[-4], refs[-3], refs[-2], refs[-1]
    rows = whole.shape[0] // size
    if len(in_refs) == 1:
        values = in_refs[0][...].reshape(whole.shape)
    else:
        for step, in_ref in enumerate(in_refs):
            source = lax.rem(me_ref[0] + size - step, size)
            whole[pl.ds(pl.multiple_of(source * rows, rows), rows)] = in_ref[0]
        values = whole[...]
    half = values.shape[0] // 2
    for parity in range(2):
        mixed = values[:half] + values[half:] if parity == 0 else values[:half] - values[half:]
        high, low = permuted_split(mixed, order_ref[...])
        result = three_dots(table_ref[parity, 0], table_ref[parity, 1], high, low)
        out_ref[:, 0, parity] = result.reshape(out_ref.shape[:1] + out_ref.shape[3:])


def forward_transform(me, arrays, tables, order, size, blocks, after):
    spread = len(arrays) > 1
    count, rows, cells_r = arrays[0].shape[-3:]
    length = size * rows
    half = length // 2
    few = half // blocks
    tiled = few % 8 == 0
    shape = (blocks, count, 2, few, cells_r) if tiled else (1, count, 2, half, cells_r)
    if spread:
        specs = [pl.BlockSpec((1, rows, cells_r), lambda z: (z, 0, 0))] * size
    else:
        specs = [pl.BlockSpec((size, 1, rows, cells_r), lambda z: (0, z, 0, 0))]
    modes = pl.pallas_call(
        placed_after(functools.partial(forward_kernel, size)),
        grid=(count,),
        in_specs=[pl.BlockSpec(memory_space=pltpu.SMEM), pl.BlockSpec(memory_space=pl.ANY)] + specs + [any_spec(tables), any_spec(order)],
        out_specs=pl.BlockSpec((shape[0], 1) + shape[2:], lambda z: (0, z, 0, 0, 0)),
        out_shape=f32_shape(*shape),
        scratch_shapes=[pltpu.VMEM((length, cells_r), jnp.float32)],
        compiler_params=params(),
        cost_estimate=sliced_cost(6 * count * length * half * cells_r, shape, shape, tables.shape),
        name="forward_transform",
    )(me, after, *arrays, tables, order)
    if not tiled:
        modes = jnp.transpose(modes.reshape(count, 2, blocks, few, cells_r), (2, 0, 1, 3, 4))
    return modes.reshape(blocks, count, 2 * few, cells_r)


def backward_kernel(size, spread, me_ref, modes_ref, table_ref, order_ref, *refs):
    out_refs, whole = refs[:-1], refs[-1]
    half, cells_r = table_ref.shape[2], whole.shape[2]
    parts = []
    for parity in range(2):
        high, low = permuted_split(modes_ref[:, 0, parity].reshape(half, cells_r), order_ref[...])
        parts.append(three_dots(table_ref[parity, 0], table_ref[parity, 1], high, low))
    shape = (size // 2,) + whole.shape[1:]
    near, far = (parts[0] + parts[1]).reshape(shape), (parts[0] - parts[1]).reshape(shape)
    if spread:
        whole[: size // 2] = near
        whole[size // 2:] = far
        for step in range(size):
            out_refs[step][0] = whole[lax.rem(me_ref[0] + step, size)]
    else:
        out_refs[0][: size // 2, 0] = near
        out_refs[0][size // 2:, 0] = far


def backward_transform(me, modes, tables, order, size, spread, after):
    blocks, count, few, cells_r = modes.shape
    length = blocks * few
    rows = length // size
    modes = modes.reshape(blocks, count, 2, few // 2, cells_r)
    if few // 2 % 8:
        modes = jnp.transpose(modes, (1, 2, 0, 3, 4)).reshape(1, count, 2, length // 2, cells_r)
    if spread:
        shapes = [f32_shape(count, rows, cells_r)] * size
        specs = [pl.BlockSpec((1, rows, cells_r), lambda z: (z, 0, 0))] * size
    else:
        shapes = [f32_shape(size, count, rows, cells_r)]
        specs = [pl.BlockSpec((size, 1, rows, cells_r), lambda z: (0, z, 0, 0))]
    return pl.pallas_call(
        placed_after(functools.partial(backward_kernel, size, spread)),
        grid=(count,),
        in_specs=[
            pl.BlockSpec(memory_space=pltpu.SMEM),
            pl.BlockSpec(memory_space=pl.ANY),
            pl.BlockSpec((modes.shape[0], 1) + modes.shape[2:], lambda z: (0, z, 0, 0, 0)),
            any_spec(tables),
            any_spec(order),
        ],
        out_specs=specs,
        out_shape=shapes,
        scratch_shapes=[pltpu.VMEM((size, rows, cells_r), jnp.float32)],
        compiler_params=params(),
        cost_estimate=sliced_cost(3 * count * length * length * cells_r, modes.shape, modes.shape, tables.shape),
        name="backward_transform",
    )(me, after, modes, tables, order)


def solve_kernel(places, outer_ref, order2_ref, ends_ref, *refs):
    chunk_refs, refs = refs[: len(places)], refs[len(places):]
    out_refs, refs = refs[: len(places)], refs[len(places):]
    scale_ref, ping, pong, source_ref, rest, fine_w, fine_d, rhs, thin, thick, coarse_w = refs
    total_z, modes, cells_r = source_ref.shape
    lanes = cells_r // 2
    total_y = total_z // 2
    tile = min(8, modes)
    tiles = modes // tile
    block_z = block_of(total_z, 64)
    block_y = block_of(total_y, 32)
    blocks_z = total_z // block_z
    blocks_y = total_y // block_y

    spot = lax.broadcasted_iota(jnp.int32, (1, lanes), 1)
    position = spot.astype(jnp.float32)
    first = spot == 0
    last = spot == lanes - 1
    fine = []
    for parity in range(2):
        radius = RIN + (2.0 * position + parity) + 0.5
        fine.append((radius, (radius - 0.5) / radius, (radius + 0.5) / radius))
    coarse_radius = RIN + 2.0 * position + 1.0
    coarse_in = (coarse_radius - 1.0) / (4.0 * coarse_radius)
    coarse_out = (coarse_radius + 1.0) / (4.0 * coarse_radius)

    def wide(row):
        return jnp.broadcast_to(row, (tile, lanes))

    in_even = wide(jnp.where(first, 0.0, fine[0][1]))
    out_even = wide(fine[0][2])
    in_odd = wide(fine[1][1])
    out_odd = wide(jnp.where(last, 0.0, fine[1][2]))
    coarse_below = wide(jnp.where(first, 0.0, coarse_in))
    coarse_above = wide(jnp.where(last, 0.0, coarse_out))
    even = pl.ds(0, lanes)
    odd = pl.ds(lanes, lanes)

    order2 = order2_ref[...]
    open_fine = [jnp.where(ends_ref[:, p * lanes:(p + 1) * lanes] == 0, 1.0, 0.0) for p in range(2)]
    extra = [order2 / (fine[p][0] * fine[p][0]) for p in range(2)]
    extra_coarse = order2 / (coarse_radius * coarse_radius)

    base_even = (fine[0][1] + fine[0][2]) + extra[0]
    base_odd = fine[1][1] + extra[1]

    def fill_fine(z, carry):
        kept = 2.0 - jnp.where(z == 0, open_fine[0], 0.0) - jnp.where(z == total_z - 1, open_fine[0], 0.0)
        full = base_even + kept
        fine_d[z, :, even] = full
        fine_w[z, :, even] = relaxation / full
        kept = 2.0 - jnp.where(z == 0, open_fine[1], 0.0) - jnp.where(z == total_z - 1, open_fine[1], 0.0)
        kept = kept + jnp.where(last & (outer_ref[z] == 0), 0.0, fine[1][2])
        full = base_odd + kept
        fine_d[z, :, odd] = full
        fine_w[z, :, odd] = relaxation / full
        return carry

    lax.fori_loop(0, total_z, fill_fine, 0)

    def fill_coarse(y, carry):
        kept = 2.0 - jnp.where(y == 0, open_fine[0], 0.0) - jnp.where(y == total_y - 1, open_fine[0], 0.0)
        kept = 0.25 * kept + (coarse_in + jnp.where(last & (outer_ref[2 * y] == 0), 0.0, coarse_out))
        coarse_w[y + 1] = relaxation / (kept + extra_coarse)
        return carry

    lax.fori_loop(0, total_y, fill_coarse, 0)

    for spots, chunk_ref in zip(places, chunk_refs):
        for block, row_spots in enumerate(spots):
            for row, z in enumerate(row_spots):
                source_ref[z] = chunk_ref[block, row]

    zero_fine = jnp.zeros((1, modes, cells_r), jnp.float32)
    zero_coarse = jnp.zeros((1, modes, lanes), jnp.float32)
    for buffer in (ping, pong):
        buffer[pl.ds(0, 1)] = zero_fine
        buffer[pl.ds(total_z + 1, 1)] = zero_fine
    for buffer in (rhs, thin, thick, coarse_w):
        buffer[pl.ds(0, 1)] = zero_coarse
        buffer[pl.ds(total_y + 1, 1)] = zero_coarse

    def each(blocks, block, body):
        def one(step, carry):
            there = pl.ds(pl.multiple_of(step // blocks * tile, tile), tile)
            body(step % blocks * block, there)
            return carry

        lax.fori_loop(0, tiles * blocks, one, 0, unroll=True)

    def neighbour_sum(rows, at):
        before_e, before_o = rows[at - 1]
        here_e, here_o = rows[at]
        after_e, after_o = rows[at + 1]
        sum_e = (before_e + after_e) + (in_even * pltpu.roll(here_o, 1, 1) + out_even * here_o)
        sum_o = (before_o + after_o) + (in_odd * here_e + out_odd * pltpu.roll(here_e, lanes - 1, 1))
        return sum_e, sum_o

    def relax_rows(rows, z0, there, store):
        for at in range(block_z):
            z = z0 + at
            sum_e, sum_o = neighbour_sum(rows, at + 1)
            here_e, here_o = rows[at + 1]
            new_e = (1.0 - relaxation) * here_e + fine_w[z, there, even] * (source_ref[z, there, even] + sum_e)
            new_o = (1.0 - relaxation) * here_o + fine_w[z, there, odd] * (source_ref[z, there, odd] + sum_o)
            store(z, there, new_e, new_o)

    def store_padded(buffer):
        def store(z, there, new_e, new_o):
            buffer[z + 1, there, even] = new_e
            buffer[z + 1, there, odd] = new_o
        return store

    def padded_rows(buffer, z0, there):
        return [(buffer[z0 + at, there, even], buffer[z0 + at, there, odd]) for at in range(block_z + 2)]

    def sweep(buffer, store):
        each(blocks_z, block_z, lambda z0, there: relax_rows(padded_rows(buffer, z0, there), z0, there, store))

    def first_sweep(store):
        def body(z0, there):
            for at in range(block_z):
                z = z0 + at
                store(z, there, fine_w[z, there, even] * source_ref[z, there, even],
                      fine_w[z, there, odd] * source_ref[z, there, odd])
        each(blocks_z, block_z, body)

    def residual_pass(buffer):
        def body(z0, there):
            rows = padded_rows(buffer, z0, there)
            pair = None
            for at in range(block_z):
                z = z0 + at
                sum_e, sum_o = neighbour_sum(rows, at + 1)
                here_e, here_o = rows[at + 1]
                left_e = (source_ref[z, there, even] + sum_e) - fine_d[z, there, even] * here_e
                left_o = (source_ref[z, there, odd] + sum_o) - fine_d[z, there, odd] * here_o
                rest[z, there, even] = left_e
                rest[z, there, odd] = left_o
                if at % 2 == 0:
                    pair = left_e + left_o
                else:
                    rhs[z0 // 2 + at // 2 + 1, there] = 0.25 * (pair + (left_e + left_o))
        each(blocks_z, block_z, body)

    def coarse_rows(load, y0, there):
        return [load(y0 + at, there) for at in range(block_y + 2)]

    def coarse_relax(load, target):
        def body(y0, there):
            rows = coarse_rows(load, y0, there)
            for at in range(block_y):
                y = y0 + at
                here = rows[at + 1]
                total = 0.25 * (rows[at] + rows[at + 2]) + (
                    coarse_below * pltpu.roll(here, 1, 1) + coarse_above * pltpu.roll(here, lanes - 1, 1))
                target[y + 1, there] = (1.0 - relaxation) * here + coarse_w[y + 1, there] * (rhs[y + 1, there] + total)
        each(blocks_y, block_y, body)

    def load_of(buffer):
        return lambda y, there: buffer[y, there]

    def load_first(y, there):
        return coarse_w[y, there] * rhs[y, there]

    def coarse_solve():
        buffers = (thin, thick)
        load = load_first
        for step in range(KC):
            target = buffers[step % 2]
            coarse_relax(load, target)
            load = load_of(target)
        return buffers[(KC - 1) % 2]

    gain_even = 1.0 + wide(fine[0][2])
    gain_odd = 1.0 + wide(fine[1][1])

    def image_scale(estimate, there):
        def one(block, carry):
            top, bottom = carry
            y0 = block * block_y
            rows = coarse_rows(load_of(estimate), y0, there)
            for at in range(block_y):
                here = rows[at + 1]
                side_e = in_even * pltpu.roll(here, 1, 1) + gain_even * here
                side_o = out_odd * pltpu.roll(here, lanes - 1, 1) + gain_odd * here
                for low in range(2):
                    z = 2 * (y0 + at) + low
                    across = rows[at + 2 * low]
                    image_e = fine_d[z, there, even] * here - (side_e + across)
                    image_o = fine_d[z, there, odd] * here - (side_o + across)
                    top = top + (rest[z, there, even] * image_e + rest[z, there, odd] * image_o)
                    bottom = bottom + (image_e * image_e + image_o * image_o)
            return top, bottom

        nothing = jnp.zeros((tile, lanes), jnp.float32)
        top, bottom = lax.fori_loop(0, blocks_y, one, (nothing, nothing))
        top = jnp.sum(top, axis=1, keepdims=True)
        bottom = jnp.sum(bottom, axis=1, keepdims=True)
        return wide(top / (bottom + small_floor))

    def corrected_sweep(buffer, estimate, cycle, store):
        def each_tile(step, carry):
            there = pl.ds(pl.multiple_of(step * tile, tile), tile)
            scale_ref[cycle, there] = image_scale(estimate, there)
            return carry

        lax.fori_loop(0, tiles, each_tile, 0)

        def body(z0, there):
            scale = scale_ref[cycle, there]
            rows = padded_rows(buffer, z0, there)
            added = [scale * estimate[z0 // 2 + at, there] for at in range(block_z // 2 + 2)]
            moved = []
            for at in range(block_z + 2):
                plus = added[(at + 1) // 2]
                moved.append((rows[at][0] + plus, rows[at][1] + plus))
            relax_rows(moved, z0, there, store)
        each(blocks_z, block_z, body)

    for cycle in range(VCYC):
        here, other = ping, pong
        left = NU
        if cycle == 0:
            first_sweep(store_padded(here))
            left = NU - 1
        for _ in range(left):
            sweep(here, store_padded(other))
            here, other = other, here
        residual_pass(here)
        estimate = coarse_solve()
        for step in range(NU):
            store = store_padded(other)
            if step == 0:
                corrected_sweep(here, estimate, cycle, store)
            else:
                sweep(here, store)
            here, other = other, here
        ping, pong = here, other

    for spots, out_ref in zip(places, out_refs):
        for block, row_spots in enumerate(spots):
            for row, z in enumerate(row_spots):
                out_ref[block, row] = ping[z + 1]

def solve_modes(chunks, places, order2, outer_held, ends):
    modes, cells_r = chunks[0].shape[2:]
    total_z = outer_held.shape[0]
    lanes = cells_r // 2
    whole = pl.BlockSpec(memory_space=pltpu.VMEM)
    fine = (total_z, modes, cells_r)
    padded = (total_z + 2, modes, cells_r)
    coarse = (total_z // 2 + 2, modes, lanes)
    outs = pl.pallas_call(
        functools.partial(solve_kernel, places),
        in_specs=[pl.BlockSpec(memory_space=pltpu.SMEM)] + [whole] * (2 + len(chunks)),
        out_specs=[whole] * (1 + len(chunks)),
        out_shape=[f32_shape(*chunk.shape) for chunk in chunks] + [f32_shape(VCYC, modes, lanes)],
        scratch_shapes=[
            pltpu.VMEM(shape, jnp.float32)
            for shape in (padded, padded, fine, fine, fine, fine, coarse, coarse, coarse, coarse)
        ],
        compiler_params=params(),
        cost_estimate=sliced_cost(120 * math.prod(fine), fine, fine),
        name="solve_modes",
    )(outer_held, order2, ends, *chunks)
    return outs[:-1], outs[-1]


def exchange(arrays, size):
    if len(arrays) == 1:
        return [lax.all_to_all(arrays[0], "phi", split_axis=0, concat_axis=0, tiled=True)]
    moved = [arrays[0]]
    for step in range(1, size):
        pairs = [(place, (place + step) % size) for place in range(size)]
        moved.append(lax.ppermute(arrays[step], "phi", pairs))
    return moved


def exchange_all(modes):
    return lax.all_to_all(modes, ("phi", "gz"), split_axis=0, concat_axis=0, tiled=True)


def body(charge, outer_held, end_held):
    phi_size = lax.axis_size("phi")
    gz_size = lax.axis_size("gz")
    devices = phi_size * gz_size
    rows, cells_z, cells_r = charge.shape
    length = rows * phi_size
    rows_z = cells_z // phi_size
    few = length // devices
    me = lax.axis_index("phi").astype(jnp.int32)[None]

    into = out_of = ((0, rows_z, False),)
    places = [
        [[g * cells_z + j * rows_z + start + row for row in range(count)] for j in range(phi_size) for g in range(gz_size)]
        for start, count, _ in into
    ]

    exact = hartley_halves(length)
    forward = jnp.asarray(exact)
    backward = lax.optimization_barrier(forward)
    backward = jnp.stack([backward[0], jnp.swapaxes(backward[1], 1, 2)])
    order = jnp.asarray(parity_order(cells_r))
    disorder = jnp.asarray(parity_order(cells_r).T)

    place = lax.axis_index("phi") * gz_size + lax.axis_index("gz")
    slots = jnp.arange(few, dtype=jnp.int32)
    own_modes = place * few + 2 * (slots % (few // 2)) + slots // (few // 2)
    mode_order = jnp.minimum(own_modes, length - own_modes).astype(jnp.float32)
    order2 = (mode_order * mode_order)[:, None]

    sent = arrange_cells(me, charge, into, phi_size)
    sources = []
    after = order2
    for arrays in sent:
        arrays = exchange(arrays, phi_size)
        modes = forward_transform(me, arrays, forward, order, phi_size, devices, after)
        after = modes
        sources.append(exchange_all(modes))

    ends = jnp.concatenate([end_held[0::2], end_held[1::2]])[None, :]
    solved, scale_lanes = solve_modes(sources, places, order2, outer_held, ends)

    natural = scale_lanes[:, :, 0].reshape(VCYC, 2, few // 2)
    natural = jnp.transpose(natural, (0, 2, 1)).reshape(VCYC, few)
    scales = lax.all_gather(natural, "gz", axis=1, tiled=True)

    groups = []
    after = order2
    for modes, (_, _, spread) in zip(solved, out_of):
        modes = exchange_all(modes)
        arrays = backward_transform(me, modes, backward, disorder, phi_size, spread, after)
        after = arrays[0]
        groups.append(exchange(arrays, phi_size))
    potential = gather_cells(me, groups, out_of, phi_size, rows, cells_z, cells_r)
    return (potential, scales)


def solution(mesh):
    in_specs = (P("phi", "gz", None), P(), P())
    out_specs = (P("phi", "gz", None), P(None, "phi"))
    return jax.shard_map(body, mesh=mesh, in_specs=in_specs, out_specs=out_specs, check_vma=False)
```
